512 devices in a mesh: wide: 64 (over z, y), narrow: 8 (over x, core).
Axes of the slice: x: 4, y: 8, z: 8, core: 2. Of those that a mesh axis runs over, the one named last changes fastest.
Arguments:
- square_grads: bfloat16 [4, 8192, 8192], P(None, 'wide', 'narrow'), may hold values from -8.1 to 8.1
- narrow_grads: bfloat16 [4, 8192, 1024], P(None, 'wide', 'narrow'), may hold values from -8.1 to 8.1
- square_rowstate: float32 [4, 8192], P(None, 'wide'), may hold values from 0.0006 to 0.064
- square_colstate: float32 [4, 8192], P(None, 'narrow'), may hold values from 1e-05 to 2.1
- narrow_rowstate: float32 [4, 8192], P(None, 'wide'), may hold values from 0.0006 to 0.064
- narrow_colstate: float32 [4, 1024], P(None, 'narrow'), may hold values from 1e-05 to 2.1
Outputs:
- square_update: float32 [4, 8192, 8192], P(None, 'wide', 'narrow')
- narrow_update: float32 [4, 8192, 1024], P(None, 'wide', 'narrow')
- square_rowfactor: float32 [4, 8192], P(None, 'wide')
- square_colfactor: float32 [4, 8192], P(None, 'narrow')
- narrow_rowfactor: float32 [4, 8192], P(None, 'wide')
- narrow_colfactor: float32 [4, 1024], P(None, 'narrow')
The draws below stay inside these ranges and needn't reach their ends.
All inputs are finite; a program needn't handle non-finite values.
Results may differ from the reference program's by a relative error of at most 0.0004.
Values sent between devices are 32-bit elements; how exact they have to be, the bound alone decides.
A program may use at most 64 MiB of HBM per device.

```python
import jax
import jax.numpy as jnp
from jax import lax

MODEL_WIDTH = 8192
KEY_VALUE_WIDTH = 1024
NSQ = 4
KEY_VALUE_COUNT = 4


def scale_profile(key, count, length, reverse):
    place = jnp.arange(length, dtype=jnp.float32) / length
    if reverse:
        place = 1.0 - place
    jitter = jax.random.uniform(key, (count, length), jnp.float32)
    return 10.0 ** (0.5 * place[None, :] + 0.5 * jitter)


def gradient_sample(key, count, length, width):
    row_scale = scale_profile(jax.random.fold_in(key, 11), count, length, False)
    col_first = scale_profile(jax.random.fold_in(key, 12), count, width, False)
    col_second = scale_profile(jax.random.fold_in(key, 15), count, width, True)
    mixing = jax.random.uniform(jax.random.fold_in(key, 16), (count, length, 1), jnp.float32)
    col_mixed = jnp.sqrt(mixing * jnp.square(col_first)[:, None, :] + (1.0 - mixing) * jnp.square(col_second)[:, None, :])
    noise = jax.random.truncated_normal(jax.random.fold_in(key, 13), -4.0, 4.0, (count, length, width), jnp.float32)
    return (0.01 * noise * row_scale[:, :, None] * col_mixed).astype(jnp.bfloat16)


def state_sample(key, count, length):
    place = jnp.arange(length, dtype=jnp.float32) / length
    noise = 10.0 ** jax.random.uniform(key, (count, length), jnp.float32, -0.5, 0.5)
    return 0.002 * (10.0 ** place)[None, :] * noise


def level_sample(key, count):
    order = jax.random.permutation(key, count)
    level_values = 10.0 ** jnp.linspace(-1.5, 1.5, count, dtype=jnp.float32)
    return level_values[order]


def draw_square_grads(key, part):
    return gradient_sample(jax.random.fold_in(key, 1), NSQ, MODEL_WIDTH, MODEL_WIDTH)


def draw_narrow_grads(key, part):
    return gradient_sample(jax.random.fold_in(key, 2), KEY_VALUE_COUNT, MODEL_WIDTH, KEY_VALUE_WIDTH)


def draw_square_rowstate(key, part):
    return state_sample(jax.random.fold_in(key, 3), NSQ, MODEL_WIDTH)


def draw_narrow_rowstate(key, part):
    return state_sample(jax.random.fold_in(key, 4), KEY_VALUE_COUNT, MODEL_WIDTH)


def draw_square_colstate(key, part):
    level_values = level_sample(jax.random.fold_in(key, 5), NSQ)
    return state_sample(jax.random.fold_in(key, 6), NSQ, MODEL_WIDTH) * level_values[:, None]


def draw_narrow_colstate(key, part):
    level_values = level_sample(jax.random.fold_in(key, 7), KEY_VALUE_COUNT)
    return state_sample(jax.random.fold_in(key, 8), KEY_VALUE_COUNT, KEY_VALUE_WIDTH) * level_values[:, None]


def setup_inputs(seed: int = 0) -> dict:
    keys = jax.random.split(jax.random.key(seed), 7)
    square_grads = draw_square_grads(jax.random.fold_in(keys[6], 71), 0)
    narrow_grads = draw_narrow_grads(jax.random.fold_in(keys[6], 71), 0)
    square_rowstate = draw_square_rowstate(jax.random.fold_in(keys[6], 71), 0)
    square_colstate = draw_square_colstate(jax.random.fold_in(keys[6], 71), 0)
    narrow_rowstate = draw_narrow_rowstate(jax.random.fold_in(keys[6], 71), 0)
    narrow_colstate = draw_narrow_colstate(jax.random.fold_in(keys[6], 71), 0)
    return dict(square_grads=square_grads, narrow_grads=narrow_grads, square_rowstate=square_rowstate, square_colstate=square_colstate, narrow_rowstate=narrow_rowstate, narrow_colstate=narrow_colstate)


decay_rate = 0.9
epsilon_square = 1e-30
clip_limit = 1.0

def one_matrix(inputs):
    grads, rowstate, colstate = inputs
    values = grads.astype(jnp.float32)
    squares = values * values + epsilon_square
    rowfactor = decay_rate * rowstate + (1.0 - decay_rate) * lax.optimization_barrier(jnp.mean(squares, axis=1))
    colfactor = decay_rate * colstate + (1.0 - decay_rate) * lax.optimization_barrier(jnp.mean(squares, axis=0))
    row_mean = jnp.mean(rowfactor)
    raw = values * lax.rsqrt(rowfactor)[:, None] * lax.rsqrt(colfactor)[None, :] * jnp.sqrt(row_mean)
    spread = jnp.sqrt(jnp.mean(raw * raw))
    update = raw / jnp.maximum(1.0, spread / clip_limit)
    return (update, rowfactor, colfactor)

def reference(square_grads, narrow_grads, square_rowstate, square_colstate, narrow_rowstate, narrow_colstate):
    square_update, square_rowfactor, square_colfactor = lax.map(one_matrix, (square_grads, square_rowstate, square_colstate))
    narrow_update, narrow_rowfactor, narrow_colfactor = lax.map(one_matrix, (narrow_grads, narrow_rowstate, narrow_colstate))
    return (square_update, narrow_update, square_rowfactor, square_colfactor, narrow_rowfactor, narrow_colfactor)
```

```python
import functools

import jax
import jax.numpy as jnp
from jax import lax
from jax.experimental import pallas as pl
from jax.experimental.pallas import tpu as pltpu
from jax.sharding import Mesh
from jax.sharding import PartitionSpec as P

WIDE = ("wide_0", "wide_1")
NARROW = ("narrow_0", "narrow_1")
MESH = pl.DeviceIdType.MESH

decay_rate = 0.9
epsilon_square = 1e-30
clip_limit = 1.0

f32 = jnp.float32

ROWS, CZ, CY, WZ, WY, AG, SZ, SN = range(8)
FAR_FIRST = (4, 3, 5, 2, 6, 1, 7)


def exchange_kernel(
    gs, gn, rs, rn, cs, cn,
    ts, tn, rowf, colfs, colfn, cscs, cscn,
    vs, vn, vrs, vrn, vcs, vcn, part, rb,
    rows_buf, c_out, w_out, cz, cy, wz, wy, ag, sz, sn,
    load_sem, send_sem, recv_sem,
):
    z, y = lax.axis_index("wide_0"), lax.axis_index("wide_1")
    x, core = lax.axis_index("narrow_0"), lax.axis_index("narrow_1")

    def on_z(d):
        return {"wide_0": lax.rem(z + d, 8)}

    def on_y(d):
        return {"wide_1": lax.rem(y + d, 8)}

    def on_narrow(d):
        return {"narrow_0": lax.rem(x + d // 2, 4), "narrow_1": lax.rem(core + d % 2, 2)}

    loads = [pltpu.make_async_copy(gs.at[m], vs.at[m], load_sem.at[m]) for m in range(4)]
    loads.append(pltpu.make_async_copy(gn, vn, load_sem.at[4]))
    for i, (a, b) in enumerate(((rs, vrs), (rn, vrn), (cs, vcs), (cn, vcn))):
        loads.append(pltpu.make_async_copy(a, b, load_sem.at[5 + i]))
    for c in loads:
        c.start()

    barrier = pltpu.get_barrier_semaphore()
    for d in FAR_FIRST:
        for peer in (on_z(d), on_y(d), on_narrow(d)):
            pl.semaphore_signal(barrier, inc=1, device_id=peer, device_id_type=MESH)

    def send(kind, d, src, dst, peer):
        c = pltpu.make_async_remote_copy(
            src_ref=src, dst_ref=dst, send_sem=send_sem.at[kind, d], recv_sem=recv_sem.at[kind, d],
            device_id=peer, device_id_type=MESH)
        c.start()
        return c

    started = []

    def column_sums(m, ref, width):
        blocks = width // 128

        def step(r, acc):
            rows = pl.ds(r * 16, 16)
            v = ref[rows, :].astype(f32)
            q = v * v
            p = q[:, 0:128]
            for b in range(1, blocks):
                p = p + q[:, b * 128:(b + 1) * 128]
            part[m, rows, :] = p
            return acc + (q[0:8] + q[8:16])

        acc = lax.fori_loop(0, 8, step, jnp.zeros((8, width), f32), unroll=True)
        return jnp.sum(acc, axis=0, keepdims=True)

    for m in range(4):
        loads[m].wait()
        total = column_sums(m, vs.at[m], 1024)
        for k in range(8):
            c_out[k, m:m + 1, :] = total[:, k * 128:(k + 1) * 128]
    loads[4].wait()
    for m in range(4):
        total = column_sums(4 + m, vn.at[m], 128)
        c_out[m, 4:5, :] = total
        c_out[m + 4, 4:5, :] = total
    for m in range(8):
        rows_buf[0, m:m + 1, :] = jnp.sum(part[m].T, axis=0, keepdims=True)

    pl.semaphore_wait(barrier, 21)

    row_copies = [send(ROWS, d, rows_buf.at[0], rows_buf.at[d], on_narrow(d)) for d in FAR_FIRST]
    cz[0] = c_out[z]
    cz_copies = [send(CZ, d, c_out.at[lax.rem(z + d, 8)], cz.at[d], on_z(d)) for d in FAR_FIRST]
    started += row_copies + cz_copies

    for c in loads[5:]:
        c.wait()

    for c in row_copies:
        c.wait_recv()
    rowsum = None
    for sx in range(4):
        for sc in range(2):
            slot = lax.rem(x + 4 - sx, 4) * 2 + lax.rem(core + sc, 2)
            piece = rows_buf[slot]
            rowsum = piece if rowsum is None else rowsum + piece
    sub = lax.broadcasted_iota(jnp.int32, (8, 128), 0)
    lane = lax.broadcasted_iota(jnp.int32, (8, 128), 1)
    rowf[0:4, :] = decay_rate * vrs[...] + (1.0 - decay_rate) * (rowsum[0:4] / 8192 + epsilon_square)
    rowf[4:8, :] = decay_rate * vrn[...] + (1.0 - decay_rate) * (rowsum[4:8] / 1024 + epsilon_square)
    factor = rowf[...]
    inverse = lax.rsqrt(factor)
    for m in range(8):
        rb[m] = jnp.broadcast_to(inverse[m:m + 1, :], (128, 128)).T
    totals = jnp.sum(factor, axis=1, keepdims=True)
    totals = jnp.sum(jnp.where(lane == sub, totals, 0.0), axis=0, keepdims=True)
    for k in range(8):
        w_out[k, 5:6, :] = totals

    def weighted_sums(m, ref, out, width):
        blocks = width // 128

        def step(r, acc):
            rows = pl.ds(r * 16, 16)
            scale = rb[m, rows, :]
            v = ref[rows, :].astype(f32)
            new = []
            for b in range(blocks):
                t = v[:, b * 128:(b + 1) * 128] * scale
                out[rows, b * 128:(b + 1) * 128] = t
                q = t * t
                new.append(acc[b] + (q[0:8] + q[8:16]))
            return tuple(new)

        acc = lax.fori_loop(0, 8, step, tuple(jnp.zeros((8, 128), f32) for _ in range(blocks)), unroll=True)
        return [jnp.sum(a, axis=0, keepdims=True) for a in acc]

    for m in range(4):
        total = weighted_sums(m, vs.at[m], ts.at[m], 1024)
        for k in range(8):
            w_out[k, m:m + 1, :] = total[k]
    for m in range(4):
        total = weighted_sums(4 + m, vn.at[m], tn.at[m], 128)[0]
        w_out[m, 4:5, :] = total
        w_out[m + 4, 4:5, :] = total

    wz[0] = w_out[z]
    wz_copies = [send(WZ, d, w_out.at[lax.rem(z + d, 8)], wz.at[d], on_z(d)) for d in FAR_FIRST]
    started += wz_copies

    def gathered(buf, me, copies):
        for c in copies:
            c.wait_recv()
        total = None
        for s in range(8):
            piece = buf[lax.rem(me + 8 - s, 8)]
            total = piece if total is None else total + piece
        return total

    cy[0] = gathered(cz, z, cz_copies)
    cy_copies = [send(CY, d, cy.at[0], cy.at[d], on_y(d)) for d in FAR_FIRST]
    started += cy_copies

    wy[0] = gathered(wz, z, wz_copies)
    wy_copies = [send(WY, d, wy.at[0], wy.at[d], on_y(d)) for d in FAR_FIRST]
    started += wy_copies

    colsum = gathered(cy, y, cy_copies)
    state = vcs[:, pl.ds(pl.multiple_of(z * 128, 128), 128)]
    ag[0, 0:4, :] = decay_rate * state + (1.0 - decay_rate) * (colsum[0:4] / 8192 + epsilon_square)
    ag[0, 4:5, :] = (decay_rate * vcn[pl.ds(lax.rem(z, 4), 1), :]
                     + (1.0 - decay_rate) * (colsum[4:5] / 8192 + epsilon_square))
    ag_copies = [send(AG, d, ag.at[0], ag.at[d], on_z(d)) for d in FAR_FIRST]
    started += ag_copies
    own = ag[0]

    weighted = gathered(wy, y, wy_copies)
    share = jnp.sum(weighted[0:5] / own, axis=1, keepdims=True)
    sub5, lane5 = sub[0:5], lane[0:5]
    target = jnp.where(sub5 == 4, 4 + z, sub5)
    share = jnp.sum(jnp.where(lane5 == target, share, 0.0), axis=0, keepdims=True)
    sz[0] = share
    sz_copies = [send(SZ, d, sz.at[0], sz.at[d], on_z(d)) for d in FAR_FIRST]
    started += sz_copies

    for c in ag_copies:
        c.wait_recv()
    for s in range(8):
        piece = ag[lax.rem(z + 8 - s, 8)]
        colfs[:, s * 128:(s + 1) * 128] = piece[0:4]
        if s < 4:
            colfn[s:s + 1, :] = piece[4:5]
    inv_s, inv_n = lax.rsqrt(colfs[...]), lax.rsqrt(colfn[...])

    sn[0] = gathered(sz, z, sz_copies)
    sn_copies = [send(SN, d, sn.at[0], sn.at[d], on_narrow(d)) for d in FAR_FIRST]
    started += sn_copies
    for c in sn_copies:
        c.wait_recv()
    norm = sn[0]
    for d in range(1, 8):
        norm = norm + sn[d]
    lane1 = lane[0:1]
    entries = jnp.where(lane1 < 4, 8192.0 * 8192.0, 8192.0 * 1024.0)
    row_mean = weighted[5:6] / 8192
    spread = jnp.sqrt(row_mean * norm / entries)
    scale = jnp.sqrt(row_mean) / jnp.maximum(1.0, spread / clip_limit)
    scale = jnp.sum(jnp.where(lane == sub, jnp.broadcast_to(scale, (8, 128)), 0.0), axis=1, keepdims=True)
    cscs[...] = inv_s * scale[0:4]
    cscn[...] = inv_n * scale[4:8]

    for c in started:
        c.wait_send()


def output_kernel(
    ts, tn, rowf, colfs, colfn, cscs, cscn,
    us, un, rfs, cfs, rfn, cfn,
    bs, bn, brs, brn, sem,
):
    brs[...] = rowf[0:4, :]
    brn[...] = rowf[4:8, :]
    copies = [
        pltpu.make_async_copy(brs, rfs, sem.at[5]),
        pltpu.make_async_copy(brn, rfn, sem.at[6]),
        pltpu.make_async_copy(colfs, cfs, sem.at[7]),
        pltpu.make_async_copy(colfn, cfn, sem.at[8]),
    ]
    for c in copies:
        c.start()
    for m in range(4):
        bs[m] = ts[m] * cscs[m:m + 1, :]
        c = pltpu.make_async_copy(bs.at[m], us.at[m], sem.at[m])
        c.start()
        copies.append(c)
    for m in range(4):
        bn[m] = tn[m] * cscn[m:m + 1, :]
    c = pltpu.make_async_copy(bn, un, sem.at[4])
    c.start()
    copies.append(c)
    for c in copies:
        c.wait()


def per_device(
    square_grads, narrow_grads, square_rowstate, square_colstate, narrow_rowstate, narrow_colstate
):
    hbm = pl.BlockSpec(memory_space=pltpu.HBM)
    vmem = pl.BlockSpec(memory_space=pltpu.VMEM)
    V = pltpu.VMEM
    middle = pl.pallas_call(
        exchange_kernel,
        out_shape=[
            jax.ShapeDtypeStruct((4, 128, 1024), f32), jax.ShapeDtypeStruct((4, 128, 128), f32),
            jax.ShapeDtypeStruct((8, 128), f32),
            jax.ShapeDtypeStruct((4, 1024), f32), jax.ShapeDtypeStruct((4, 128), f32),
            jax.ShapeDtypeStruct((4, 1024), f32), jax.ShapeDtypeStruct((4, 128), f32),
        ],
        in_specs=[hbm] * 6,
        out_specs=[vmem] * 7,
        scratch_shapes=[
            V((4, 128, 1024), jnp.bfloat16), V((4, 128, 128), jnp.bfloat16),
            V((4, 128), f32), V((4, 128), f32), V((4, 1024), f32), V((4, 128), f32),
            V((8, 128, 128), f32), V((8, 128, 128), f32),
            V((8, 8, 128), f32),
            V((8, 5, 128), f32), V((8, 6, 128), f32),
            V((8, 5, 128), f32), V((8, 5, 128), f32),
            V((8, 6, 128), f32), V((8, 6, 128), f32),
            V((8, 5, 128), f32), V((8, 1, 128), f32), V((8, 1, 128), f32),
            pltpu.SemaphoreType.DMA((9,)),
            pltpu.SemaphoreType.DMA((8, 8)),
            pltpu.SemaphoreType.DMA((8, 8)),
        ],
        compiler_params=pltpu.CompilerParams(
            collective_id=0, has_side_effects=True, vmem_limit_bytes=24 * 2**20),
        name="exchange",
    )(*(pltpu.with_memory_space_constraint(a, pltpu.HBM) for a in (
        square_grads, narrow_grads, square_rowstate, narrow_rowstate, square_colstate, narrow_colstate)))
    us, un, rfs, cfs, rfn, cfn = pl.pallas_call(
        output_kernel,
        out_shape=[
            jax.ShapeDtypeStruct((4, 128, 1024), f32), jax.ShapeDtypeStruct((4, 128, 128), f32),
            jax.ShapeDtypeStruct((4, 128), f32), jax.ShapeDtypeStruct((4, 1024), f32),
            jax.ShapeDtypeStruct((4, 128), f32), jax.ShapeDtypeStruct((4, 128), f32),
        ],
        in_specs=[vmem] * 7,
        out_specs=[hbm] * 6,
        scratch_shapes=[
            V((4, 128, 1024), f32), V((4, 128, 128), f32), V((4, 128), f32), V((4, 128), f32),
            pltpu.SemaphoreType.DMA((9,)),
        ],
        compiler_params=pltpu.CompilerParams(vmem_limit_bytes=24 * 2**20),
        name="output",
    )(*middle)
    return us, un, rfs, cfs, rfn, cfn


def solution(mesh):
    torus = Mesh(mesh.devices.reshape(8, 8, 4, 2), ("wide_0", "wide_1", "narrow_0", "narrow_1"))
    in_specs = (
        P(None, WIDE, NARROW),
        P(None, WIDE, NARROW),
        P(None, WIDE),
        P(None, NARROW),
        P(None, WIDE),
        P(None, NARROW),
    )
    out_specs = (
        P(None, WIDE, NARROW),
        P(None, WIDE, NARROW),
        P(None, WIDE),
        P(None, NARROW),
        P(None, WIDE),
        P(None, NARROW),
    )
    return jax.shard_map(
        per_device, mesh=torus, in_specs=in_specs, out_specs=out_specs, check_vma=False
    )
```

```python
import functools

import jax
import jax.numpy as jnp
from jax import lax
from jax.experimental import pallas as pl
from jax.experimental.pallas import tpu as pltpu
from jax.sharding import Mesh
from jax.sharding import PartitionSpec as P

WIDE = ("wide_0", "wide_1")
NARROW = ("narrow_0", "narrow_1")
MESH = pl.DeviceIdType.MESH

decay_rate = 0.9
epsilon_square = 1e-30
clip_limit = 1.0

f32 = jnp.float32

ROWS, CZ, CY, WZ, WY, AG, SX = range(7)
FAR_FIRST = (4, 3, 5, 2, 6, 1, 7)

OWNERS = 4
OFFSET = 0
BLOCKS = 8 // OWNERS
NARROWS = max(1, 4 // OWNERS)
CR = 4 * BLOCKS + NARROWS
WR = CR + 1


def exchange_kernel(
    gs, gn, rs, rn, cs, cn,
    ts, tn, rowf, colfs, colfn, cscs, cscn,
    vs, vn, vrs, vrn, vcs, vcn, part, rb,
    rows_buf, c_out, w_out, cz, cy, wz, wy, own, ag, sx,
    load_sem, send_sem, recv_sem,
):
    z, y = lax.axis_index("wide_0"), lax.axis_index("wide_1")
    x, core = lax.axis_index("narrow_0"), lax.axis_index("narrow_1")
    me = lax.rem(z + OFFSET, 8)
    is_owner = me < OWNERS

    def on_z(d):
        return {"wide_0": lax.rem(z + d, 8)}

    def on_y(d):
        return {"wide_1": lax.rem(y + d, 8)}

    def on_narrow(d):
        return {"narrow_0": lax.rem(x + d // 2, 4), "narrow_1": lax.rem(core + d % 2, 2)}

    loads = [pltpu.make_async_copy(gs.at[m], vs.at[m], load_sem.at[m]) for m in range(4)]
    loads.append(pltpu.make_async_copy(gn, vn, load_sem.at[4]))
    for i, (a, b) in enumerate(((rs, vrs), (rn, vrn), (cs, vcs), (cn, vcn))):
        loads.append(pltpu.make_async_copy(a, b, load_sem.at[5 + i]))

    for c in loads:
        c.start()

    barrier = pltpu.get_barrier_semaphore()
    for d in FAR_FIRST:
        pl.semaphore_signal(barrier, inc=1, device_id=on_narrow(d), device_id_type=MESH)

    @pl.when(is_owner)
    def _():
        for d in FAR_FIRST:
            pl.semaphore_signal(barrier, inc=1, device_id=on_z(d), device_id_type=MESH)
        for d in FAR_FIRST:
            pl.semaphore_signal(barrier, inc=1, device_id=on_y(d), device_id_type=MESH)

    def send(kind, src, dst, peer):
        pltpu.make_async_remote_copy(
            src_ref=src, dst_ref=dst, send_sem=send_sem.at[kind], recv_sem=recv_sem.at[kind],
            device_id=peer, device_id_type=MESH).start()

    def drained(kind, ref):
        pltpu.make_async_remote_copy(
            src_ref=ref, dst_ref=ref, send_sem=send_sem.at[kind], recv_sem=recv_sem.at[kind],
            device_id=on_z(1), device_id_type=MESH).wait_send()

    def arrived(kind, ref):
        pltpu.make_async_remote_copy(
            src_ref=ref, dst_ref=ref, send_sem=send_sem.at[kind], recv_sem=recv_sem.at[kind],
            device_id=on_z(1), device_id_type=MESH).wait_recv()

    def to_owners(kind, out, buf):
        for o in range(OWNERS):
            at = (o - OFFSET) % 8
            slot = lax.rem(at + 8 - z, 8)

            @pl.when(z != at)
            def _():
                send(kind, out.at[o], buf.at[slot], {"wide_0": at})

    def drained_owners(kind, out):
        @pl.when(is_owner)
        def _():
            drained(kind, out.at[pl.ds(0, OWNERS - 1)])

        if OWNERS < 8:
            @pl.when(jnp.logical_not(is_owner))
            def _():
                drained(kind, out)

    def total_of(buf, place):
        total = None
        for s in range(8):
            piece = buf[lax.rem(place + 8 - s, 8)]
            total = piece if total is None else total + piece
        return total

    def column_sums(m, ref, width):
        blocks = width // 128

        def step(r, acc):
            rows = pl.ds(r * 16, 16)
            v = ref[rows, :].astype(f32)
            q = v * v
            p = q[:, 0:128]
            for b in range(1, blocks):
                p = p + q[:, b * 128:(b + 1) * 128]
            part[m, rows, :] = p
            return acc + (q[0:8] + q[8:16])

        acc = lax.fori_loop(0, 8, step, jnp.zeros((8, width), f32), unroll=True)
        return jnp.sum(acc, axis=0, keepdims=True)

    def place_square(out, m, k, row):
        r = (k % BLOCKS) * 4 + m
        out[k // BLOCKS, r:r + 1, :] = row

    def place_narrow(out, m, row):
        for o in range(OWNERS):
            for i in range(NARROWS):
                if (o * NARROWS + i) % 4 == m:
                    out[o, 4 * BLOCKS + i:4 * BLOCKS + i + 1, :] = row

    for m in range(4):
        loads[m].wait()
        total = column_sums(m, vs.at[m], 1024)
        for k in range(8):
            place_square(c_out, m, k, total[:, k * 128:(k + 1) * 128])
    loads[4].wait()
    for m in range(4):
        place_narrow(c_out, m, column_sums(4 + m, vn.at[m], 128))
    for m in range(8):
        rows_buf[0, m:m + 1, :] = jnp.sum(part[m].T, axis=0, keepdims=True)
    for c in loads[5:]:
        c.wait()

    pl.semaphore_wait(barrier, jnp.where(is_owner, 7 + OWNERS - 1 + 7, 7 + OWNERS))

    for d in FAR_FIRST:
        send(ROWS, rows_buf.at[0], rows_buf.at[d], on_narrow(d))
    to_owners(CZ, c_out, cz)

    arrived(ROWS, rows_buf.at[pl.ds(1, 7)])
    rowsum = None
    for s_x in range(4):
        for s_c in range(2):
            slot = lax.rem(x + 4 - s_x, 4) * 2 + lax.rem(core + s_c, 2)
            piece = rows_buf[slot]
            rowsum = piece if rowsum is None else rowsum + piece
    sub = lax.broadcasted_iota(jnp.int32, (8, 128), 0)
    lane = lax.broadcasted_iota(jnp.int32, (8, 128), 1)
    rowf[0:4, :] = decay_rate * vrs[...] + (1.0 - decay_rate) * (rowsum[0:4] / 8192 + epsilon_square)
    rowf[4:8, :] = decay_rate * vrn[...] + (1.0 - decay_rate) * (rowsum[4:8] / 1024 + epsilon_square)
    factor = rowf[...]
    inverse = lax.rsqrt(factor)
    for m in range(8):
        rb[m] = jnp.broadcast_to(inverse[m:m + 1, :], (128, 128)).T
    totals = jnp.sum(factor, axis=1, keepdims=True)
    totals = jnp.sum(jnp.where(lane == sub, totals, 0.0), axis=0, keepdims=True)
    for o in range(OWNERS):
        w_out[o, CR:CR + 1, :] = totals

    def weighted_sums(m, ref, out, width):
        blocks = width // 128

        def step(r, acc):
            rows = pl.ds(r * 16, 16)
            scale = rb[m, rows, :]
            v = ref[rows, :].astype(f32)
            new = []
            for b in range(blocks):
                t = v[:, b * 128:(b + 1) * 128] * scale
                out[rows, b * 128:(b + 1) * 128] = t
                q = t * t
                new.append(acc[b] + (q[0:8] + q[8:16]))
            return tuple(new)

        acc = lax.fori_loop(0, 8, step, tuple(jnp.zeros((8, 128), f32) for _ in range(blocks)), unroll=True)
        return [jnp.sum(a, axis=0, keepdims=True) for a in acc]

    for m in range(4):
        total = weighted_sums(m, vs.at[m], ts.at[m], 1024)
        for k in range(8):
            place_square(w_out, m, k, total[k])
    for m in range(4):
        place_narrow(w_out, m, weighted_sums(4 + m, vn.at[m], tn.at[m], 128)[0])
    to_owners(WZ, w_out, wz)

    @pl.when(is_owner)
    def _():
        cz[0] = c_out[me]
        wz[0] = w_out[me]
        arrived(CZ, cz.at[pl.ds(1, 7)])
        cy[0] = total_of(cz, z)
        for d in FAR_FIRST:
            send(CY, cy.at[0], cy.at[d], on_y(d))
        arrived(WZ, wz.at[pl.ds(1, 7)])
        wy[0] = total_of(wz, z)
        for d in FAR_FIRST:
            send(WY, wy.at[0], wy.at[d], on_y(d))

        arrived(CY, cy.at[pl.ds(1, 7)])
        colsum = total_of(cy, y) / 8192 + epsilon_square
        for b in range(BLOCKS):
            start = pl.multiple_of((me * BLOCKS + b) * 128, 128)
            own[0, 4 * b:4 * b + 4, :] = (
                decay_rate * vcs[:, pl.ds(start, 128)] + (1.0 - decay_rate) * colsum[4 * b:4 * b + 4])
        for i in range(NARROWS):
            r = 4 * BLOCKS + i
            own[0, r:r + 1, :] = (
                decay_rate * vcn[pl.ds(lax.rem(me * NARROWS + i, 4), 1), :]
                + (1.0 - decay_rate) * colsum[r:r + 1])
        for d in FAR_FIRST:
            send(AG, own.at[0], ag.at[me], on_z(d))
        colfactor = own[0]
        ag[me] = colfactor

        arrived(WY, wy.at[pl.ds(1, 7)])
        weighted = total_of(wy, y)
        share = jnp.sum(weighted[0:CR] / colfactor, axis=1, keepdims=True)
        subc = lax.broadcasted_iota(jnp.int32, (CR, 128), 0)
        lanec = lax.broadcasted_iota(jnp.int32, (CR, 128), 1)
        target = jnp.where(subc >= 4 * BLOCKS, subc - 4 * BLOCKS + 4 + me * NARROWS, lax.rem(subc, 4))
        share = jnp.sum(jnp.where(lanec == target, share, 0.0), axis=0, keepdims=True)
        means = jnp.where(me == 0, pltpu.roll(weighted[CR:CR + 1], 16, 1), 0.0)
        sx[me * 8] = share + means
        for dz in (0,) + FAR_FIRST[::-1]:
            for d in FAR_FIRST + (0,):
                if (dz, d) != (0, 0):
                    peer = {**on_z(dz), **on_narrow(d)}
                    send(SX, sx.at[me * 8], sx.at[me * 8 + d], peer)

    @pl.when(is_owner)
    def _():
        arrived(AG, ag.at[pl.ds(0, OWNERS - 1)])

    if OWNERS < 8:
        @pl.when(jnp.logical_not(is_owner))
        def _():
            arrived(AG, ag)

    for o in range(OWNERS):
        piece = ag[o]
        for b in range(BLOCKS):
            k = o * BLOCKS + b
            colfs[:, k * 128:(k + 1) * 128] = piece[4 * b:4 * b + 4]
        for i in range(NARROWS):
            if o * NARROWS + i < 4:
                colfn[o * NARROWS + i:o * NARROWS + i + 1, :] = piece[4 * BLOCKS + i:4 * BLOCKS + i + 1]
    inv_s, inv_n = lax.rsqrt(colfs[...]), lax.rsqrt(colfn[...])

    @pl.when(is_owner)
    def _():
        arrived(SX, sx.at[pl.ds(0, 8 * OWNERS - 1)])

    if OWNERS < 8:
        @pl.when(jnp.logical_not(is_owner))
        def _():
            arrived(SX, sx)

    norm = sx[0]
    for i in range(1, 8 * OWNERS):
        norm = norm + sx[i]
    lane1 = lane[0:1]
    entries = jnp.where(lane1 < 4, 8192.0 * 8192.0, 8192.0 * 1024.0)
    row_mean = pltpu.roll(norm, 128 - 16, 1) / (8 * 8192)
    spread = jnp.sqrt(row_mean * norm / entries)
    scale = jnp.sqrt(row_mean) / jnp.maximum(1.0, spread / clip_limit)
    scale = jnp.sum(jnp.where(lane == sub, jnp.broadcast_to(scale, (8, 128)), 0.0), axis=1, keepdims=True)
    cscs[...] = inv_s * scale[0:4]
    cscn[...] = inv_n * scale[4:8]

    drained(ROWS, rows_buf.at[pl.ds(1, 7)])
    drained_owners(CZ, c_out)
    drained_owners(WZ, w_out)

    @pl.when(is_owner)
    def _():
        drained(CY, cy.at[pl.ds(1, 7)])
        drained(WY, wy.at[pl.ds(1, 7)])
        drained(AG, cy.at[pl.ds(1, 7)])
        drained(SX, part.at[0, pl.ds(0, 63)])


def output_kernel(
    ts, tn, rowf, colfs, colfn, cscs, cscn,
    us, un, rfs, cfs, rfn, cfn,
    bs, bn, brs, brn, sem,
):
    brs[...] = rowf[0:4, :]
    brn[...] = rowf[4:8, :]
    copies = [
        pltpu.make_async_copy(brs, rfs, sem.at[5]),
        pltpu.make_async_copy(brn, rfn, sem.at[6]),
        pltpu.make_async_copy(colfs, cfs, sem.at[7]),
        pltpu.make_async_copy(colfn, cfn, sem.at[8]),
    ]
    for c in copies:
        c.start()
    for m in range(4):
        bs[m] = ts[m] * cscs[m:m + 1, :]
        c = pltpu.make_async_copy(bs.at[m], us.at[m], sem.at[m])
        c.start()
        copies.append(c)
    for m in range(4):
        bn[m] = tn[m] * cscn[m:m + 1, :]
    c = pltpu.make_async_copy(bn, un, sem.at[4])
    c.start()
    copies.append(c)
    for c in copies:
        c.wait()


def per_device(
    square_grads, narrow_grads, square_rowstate, square_colstate, narrow_rowstate, narrow_colstate
):
    hbm = pl.BlockSpec(memory_space=pltpu.HBM)
    vmem = pl.BlockSpec(memory_space=pltpu.VMEM)
    V = pltpu.VMEM
    middle = pl.pallas_call(
        exchange_kernel,
        out_shape=[
            jax.ShapeDtypeStruct((4, 128, 1024), f32), jax.ShapeDtypeStruct((4, 128, 128), f32),
            jax.ShapeDtypeStruct((8, 128), f32),
            jax.ShapeDtypeStruct((4, 1024), f32), jax.ShapeDtypeStruct((4, 128), f32),
            jax.ShapeDtypeStruct((4, 1024), f32), jax.ShapeDtypeStruct((4, 128), f32),
        ],
        in_specs=[hbm] * 6,
        out_specs=[vmem] * 7,
        scratch_shapes=[
            V((4, 128, 1024), jnp.bfloat16), V((4, 128, 128), jnp.bfloat16),
            V((4, 128), f32), V((4, 128), f32), V((4, 1024), f32), V((4, 128), f32),
            V((8, 128, 128), f32), V((8, 128, 128), f32),
            V((8, 8, 128), f32),
            V((OWNERS, CR, 128), f32), V((OWNERS, WR, 128), f32),
            V((8, CR, 128), f32), V((8, CR, 128), f32),
            V((8, WR, 128), f32), V((8, WR, 128), f32),
            V((1, CR, 128), f32), V((OWNERS, CR, 128), f32),
            V((8 * OWNERS, 1, 128), f32),
            pltpu.SemaphoreType.DMA((9,)),
            pltpu.SemaphoreType.DMA((7,)),
            pltpu.SemaphoreType.DMA((7,)),
        ],
        compiler_params=pltpu.CompilerParams(
            collective_id=0, has_side_effects=True, vmem_limit_bytes=24 * 2**20),
        name="exchange",
    )(*(pltpu.with_memory_space_constraint(a, pltpu.HBM) for a in (
        square_grads, narrow_grads, square_rowstate, narrow_rowstate, square_colstate, narrow_colstate)))
    us, un, rfs, cfs, rfn, cfn = pl.pallas_call(
        output_kernel,
        out_shape=[
            jax.ShapeDtypeStruct((4, 128, 1024), f32), jax.ShapeDtypeStruct((4, 128, 128), f32),
            jax.ShapeDtypeStruct((4, 128), f32), jax.ShapeDtypeStruct((4, 1024), f32),
            jax.ShapeDtypeStruct((4, 128), f32), jax.ShapeDtypeStruct((4, 128), f32),
        ],
        in_specs=[vmem] * 7,
        out_specs=[hbm] * 6,
        scratch_shapes=[
            V((4, 128, 1024), f32), V((4, 128, 128), f32), V((4, 128), f32), V((4, 128), f32),
            pltpu.SemaphoreType.DMA((9,)),
        ],
        compiler_params=pltpu.CompilerParams(vmem_limit_bytes=24 * 2**20),
        name="output",
    )(*middle)
    return us, un, rfs, cfs, rfn, cfn


def solution(mesh):
    torus = Mesh(mesh.devices.reshape(8, 8, 4, 2), ("wide_0", "wide_1", "narrow_0", "narrow_1"))
    in_specs = (
        P(None, WIDE, NARROW),
        P(None, WIDE, NARROW),
        P(None, WIDE),
        P(None, NARROW),
        P(None, WIDE),
        P(None, NARROW),
    )
    out_specs = (
        P(None, WIDE, NARROW),
        P(None, WIDE, NARROW),
        P(None, WIDE),
        P(None, NARROW),
        P(None, WIDE),
        P(None, NARROW),
    )
    return jax.shard_map(
        per_device, mesh=torus, in_specs=in_specs, out_specs=out_specs, check_vma=False
    )
```

```python
import functools

import jax
import jax.numpy as jnp
from jax import lax
from jax.experimental import pallas as pl
from jax.experimental.pallas import tpu as pltpu
from jax.sharding import Mesh
from jax.sharding import PartitionSpec as P

WIDE = ("wide_0", "wide_1")
NARROW = ("narrow_0", "narrow_1")
MESH = pl.DeviceIdType.MESH

decay_rate = 0.9
epsilon_square = 1e-30
clip_limit = 1.0

f32 = jnp.float32

ROWS, CZ, CY, WZ, WY, AG, SX = range(7)
FAR_FIRST = (4, 3, 5, 2, 6, 1, 7)

OWNERS = 4
OFFSET = 0
BLOCKS = 8 // OWNERS
NARROWS = max(1, 4 // OWNERS)
SQ = 4 * BLOCKS
CR = SQ + NARROWS
WR = CR + 1
CR2 = 2 * CR
WR2 = CR2 + 1


def exchange_kernel(
    gs, gn, rs, rn, cs, cn,
    ts, tn, rowf, colfs, colfn, cscs, cscn,
    vs, vn, vrs, vrn, vcs, vcn, part, rb,
    rows_buf, c_out, w_out, cz, cy, wz, wy, own, ag, sx,
    load_sem, send_sem, recv_sem,
):
    z, y = lax.axis_index("wide_0"), lax.axis_index("wide_1")
    x, core = lax.axis_index("narrow_0"), lax.axis_index("narrow_1")
    me = lax.rem(z + OFFSET, 8)
    on_plane = me < OWNERS
    is_owner = jnp.logical_and(on_plane, core == 1)

    def on_y(d):
        return {"wide_1": lax.rem(y + d, 8)}

    def on_narrow(d):
        return {"narrow_0": lax.rem(x + d // 2, 4), "narrow_1": lax.rem(core + d % 2, 2)}

    barrier = pltpu.get_barrier_semaphore()
    for d in FAR_FIRST:
        pl.semaphore_signal(barrier, inc=1, device_id=on_narrow(d), device_id_type=MESH)

    loads = [pltpu.make_async_copy(gs.at[m], vs.at[m], load_sem.at[m]) for m in range(4)]
    loads.append(pltpu.make_async_copy(gn, vn, load_sem.at[4]))
    for i, (a, b) in enumerate(((rs, vrs), (rn, vrn), (cs, vcs), (cn, vcn))):
        loads.append(pltpu.make_async_copy(a, b, load_sem.at[5 + i]))
    for c in loads:
        c.start()

    @pl.when(is_owner)
    def _():
        for d in FAR_FIRST:
            for c in range(2):
                peer = {"wide_0": lax.rem(z + d, 8), "narrow_1": c}
                pl.semaphore_signal(barrier, inc=1, device_id=peer, device_id_type=MESH)
        for d in FAR_FIRST:
            pl.semaphore_signal(barrier, inc=1, device_id=on_y(d), device_id_type=MESH)

    def send(kind, src, dst, peer):
        pltpu.make_async_remote_copy(
            src_ref=src, dst_ref=dst, send_sem=send_sem.at[kind], recv_sem=recv_sem.at[kind],
            device_id=peer, device_id_type=MESH).start()

    def drained(kind, ref):
        pltpu.make_async_remote_copy(
            src_ref=ref, dst_ref=ref, send_sem=send_sem.at[kind], recv_sem=recv_sem.at[kind],
            device_id=on_y(1), device_id_type=MESH).wait_send()

    def arrived(kind, ref):
        pltpu.make_async_remote_copy(
            src_ref=ref, dst_ref=ref, send_sem=send_sem.at[kind], recv_sem=recv_sem.at[kind],
            device_id=on_y(1), device_id_type=MESH).wait_recv()

    def if_owner(then, otherwise):
        pl.when(is_owner)(then)
        pl.when(jnp.logical_not(is_owner))(otherwise)

    def to_owners(kind, out, buf):
        for o in range(OWNERS):
            at = (o - OFFSET) % 8

            @pl.when(jnp.logical_or(z != at, core == 0))
            def _():
                send(kind, out.at[o], buf.at[z * 2 + core], {"wide_0": at, "narrow_1": 1})

    def column_sums(m, ref, width):
        blocks = width // 128

        def step(r, acc):
            rows = pl.ds(r * 16, 16)
            v = ref[rows, :].astype(f32)
            q = v * v
            p = q[:, 0:128]
            for b in range(1, blocks):
                p = p + q[:, b * 128:(b + 1) * 128]
            part[m, rows, :] = p
            return acc + (q[0:8] + q[8:16])

        acc = lax.fori_loop(0, 8, step, jnp.zeros((8, width), f32), unroll=True)
        return jnp.sum(acc, axis=0, keepdims=True)

    def place_square(out, m, k, row):
        r = (k % BLOCKS) * 4 + m
        out[k // BLOCKS, r:r + 1, :] = row

    def place_narrow(out, m, row):
        for o in range(OWNERS):
            for i in range(NARROWS):
                if (o * NARROWS + i) % 4 == m:
                    out[o, SQ + i:SQ + i + 1, :] = row

    old = decay_rate / (1.0 - decay_rate) * 8192 / 64
    for m in range(4):
        loads[m].wait()
        if m == 0:
            for c in loads[5:]:
                c.wait()
        total = column_sums(m, vs.at[m], 1024) + old * vcs[m:m + 1, :]
        for k in range(8):
            place_square(c_out, m, k, total[:, k * 128:(k + 1) * 128])
    loads[4].wait()
    for m in range(4):
        place_narrow(c_out, m, column_sums(4 + m, vn.at[m], 128) + old * vcn[m:m + 1, :])
    for m in range(8):
        rows_buf[0, m:m + 1, :] = jnp.sum(part[m].T, axis=0, keepdims=True)

    others = jnp.where(on_plane, OWNERS - 1, OWNERS)
    pl.semaphore_wait(barrier, 7 + others + jnp.where(is_owner, 7, 0))

    for d in FAR_FIRST:
        send(ROWS, rows_buf.at[0], rows_buf.at[d], on_narrow(d))
    to_owners(CZ, c_out, cz)

    arrived(ROWS, rows_buf.at[pl.ds(1, 7)])
    rowsum = None
    for s_x in range(4):
        for s_c in range(2):
            slot = lax.rem(x + 4 - s_x, 4) * 2 + lax.rem(core + s_c, 2)
            piece = rows_buf[slot]
            rowsum = piece if rowsum is None else rowsum + piece
    sub = lax.broadcasted_iota(jnp.int32, (8, 128), 0)
    lane = lax.broadcasted_iota(jnp.int32, (8, 128), 1)
    rowf[0:4, :] = decay_rate * vrs[...] + (1.0 - decay_rate) * (rowsum[0:4] / 8192 + epsilon_square)
    rowf[4:8, :] = decay_rate * vrn[...] + (1.0 - decay_rate) * (rowsum[4:8] / 1024 + epsilon_square)
    factor = rowf[...]
    inverse = lax.rsqrt(factor)
    for m in range(8):
        rb[m] = jnp.broadcast_to(inverse[m:m + 1, :], (128, 128)).T
    totals = jnp.sum(factor, axis=1, keepdims=True)
    totals = jnp.sum(jnp.where(lane == sub, totals, 0.0), axis=0, keepdims=True)
    for o in range(OWNERS):
        w_out[o, CR:CR + 1, :] = totals

    def weighted_sums(m, ref, out, width):
        blocks = width // 128

        def step(r, acc):
            rows = pl.ds(r * 16, 16)
            scale = rb[m, rows, :]
            v = ref[rows, :].astype(f32)
            new = []
            for b in range(blocks):
                t = v[:, b * 128:(b + 1) * 128] * scale
                out[rows, b * 128:(b + 1) * 128] = t
                q = t * t
                new.append(acc[b] + (q[0:8] + q[8:16]))
            return tuple(new)

        acc = lax.fori_loop(0, 8, step, tuple(jnp.zeros((8, 128), f32) for _ in range(blocks)), unroll=True)
        return [jnp.sum(a, axis=0, keepdims=True) for a in acc]

    for m in range(4):
        total = weighted_sums(m, vs.at[m], ts.at[m], 1024)
        for k in range(8):
            place_square(w_out, m, k, total[k])
    for m in range(4):
        place_narrow(w_out, m, weighted_sums(4 + m, vn.at[m], tn.at[m], 128)[0])
    to_owners(WZ, w_out, wz)

    def over_z(kind, out, buf, into):
        arrived(kind, buf.at[pl.ds(0, 15)])
        for c in range(2):
            total = None
            for s in range(8):
                piece = jnp.where(jnp.logical_and(z == s, c == 1), out[me], buf[2 * s + c])
                total = piece if total is None else total + piece
            into[y, SQ * c:SQ * c + SQ, :] = total[0:SQ]
            into[y, 2 * SQ + NARROWS * c:2 * SQ + NARROWS * (c + 1), :] = total[SQ:CR]
        if kind == WZ:
            into[y, CR2:WR2, :] = total[CR:WR]

    def over_y(kind, buf):
        arrived(kind, buf.at[pl.ds(0, 7)])
        total = buf[0]
        for s in range(1, 8):
            total = total + buf[s]
        return total

    @pl.when(is_owner)
    def _():
        over_z(CZ, c_out, cz, cy)
        for d in FAR_FIRST:
            send(CY, cy.at[y], cy.at[y], on_y(d))
        over_z(WZ, w_out, wz, wy)
        for d in FAR_FIRST:
            send(WY, wy.at[y], wy.at[y], on_y(d))

        colfactor = (1.0 - decay_rate) * (over_y(CY, cy) / 8192 + epsilon_square)
        for c in range(2):
            own[c, 0:SQ, :] = colfactor[SQ * c:SQ * c + SQ]
            own[c, SQ:CR, :] = colfactor[2 * SQ + NARROWS * c:2 * SQ + NARROWS * (c + 1)]
        for d in FAR_FIRST + (0,):
            for c in range(2):
                if (d, c) != (0, 1):
                    send(AG, own.at[c], ag.at[me], {"wide_0": lax.rem(z + d, 8), "narrow_1": c})
        ag[me] = own[1]

        weighted = over_y(WY, wy)
        share = jnp.sum(weighted[0:CR2] / colfactor, axis=1, keepdims=True)
        subc = lax.broadcasted_iota(jnp.int32, (CR2, 128), 0)
        lanec = lax.broadcasted_iota(jnp.int32, (CR2, 128), 1)
        narrow = 4 + me * NARROWS + lax.rem(subc - 2 * SQ, NARROWS)
        target = jnp.where(subc >= 2 * SQ, narrow, lax.rem(subc, 4))
        sx[me * 4 + x, 0:1, :] = jnp.sum(jnp.where(lanec == target, share, 0.0), axis=0, keepdims=True)
        sx[me * 4 + x, 1:2, :] = weighted[CR2:WR2]
        mine = sx.at[me * 4 + x]
        for t_z in (0, 1, 7, 2, 6, 3, 5, 4):
            for t_x in (0, 1, 3, 2):
                for t_c in (1, 0):
                    peer = {"wide_0": t_z, "narrow_0": t_x, "narrow_1": t_c}
                    if t_c == 0:
                        send(SX, mine, mine, peer)
                    else:
                        @pl.when(jnp.logical_or(z != t_z, x != t_x))
                        def _():
                            send(SX, mine, mine, peer)

    if_owner(lambda: arrived(AG, ag.at[pl.ds(0, OWNERS - 1)]), lambda: arrived(AG, ag))
    for o in range(OWNERS):
        piece = ag[o]
        for b in range(BLOCKS):
            k = o * BLOCKS + b
            colfs[:, k * 128:(k + 1) * 128] = piece[4 * b:4 * b + 4]
        for i in range(NARROWS):
            if o * NARROWS + i < 4:
                colfn[o * NARROWS + i:o * NARROWS + i + 1, :] = piece[SQ + i:SQ + i + 1]
    inv_s, inv_n = lax.rsqrt(colfs[...]), lax.rsqrt(colfn[...])

    if_owner(lambda: arrived(SX, sx.at[pl.ds(0, 4 * OWNERS - 1)]), lambda: arrived(SX, sx))
    pair = sx[0]
    for i in range(1, 4 * OWNERS):
        pair = pair + sx[i]
    entries = jnp.where(lane[0:1] < 4, 8192.0 * 8192.0, 8192.0 * 1024.0)
    row_mean = pair[1:2] / (4 * OWNERS * 8192)
    spread = jnp.sqrt(row_mean * pair[0:1] / entries)
    scale = jnp.sqrt(row_mean) / jnp.maximum(1.0, spread / clip_limit)
    scale = jnp.sum(jnp.where(lane == sub, jnp.broadcast_to(scale, (8, 128)), 0.0), axis=1, keepdims=True)
    cscs[...] = inv_s * scale[0:4]
    cscn[...] = inv_n * scale[4:8]

    drained(ROWS, rows_buf.at[pl.ds(1, 7)])

    def drain_owner():
        drained(CZ, c_out.at[pl.ds(0, OWNERS - 1)])
        drained(WZ, w_out.at[pl.ds(0, OWNERS - 1)])
        drained(CY, cy.at[pl.ds(0, 7)])
        drained(WY, wy.at[pl.ds(0, 7)])
        drained(AG, cz.at[pl.ds(0, 15)])
        drained(SX, part.at[0, pl.ds(0, 126)])

    def drain_other():
        drained(CZ, c_out)
        drained(WZ, w_out)

    if_owner(drain_owner, drain_other)


def output_kernel(
    ts, tn, rowf, colfs, colfn, cscs, cscn,
    us, un, rfs, cfs, rfn, cfn,
    bs, bn, brs, brn, sem,
):
    brs[...] = rowf[0:4, :]
    brn[...] = rowf[4:8, :]
    copies = [
        pltpu.make_async_copy(brs, rfs, sem.at[5]),
        pltpu.make_async_copy(brn, rfn, sem.at[6]),
        pltpu.make_async_copy(colfs, cfs, sem.at[7]),
        pltpu.make_async_copy(colfn, cfn, sem.at[8]),
    ]
    for c in copies:
        c.start()
    for m in range(4):
        bs[m] = ts[m] * cscs[m:m + 1, :]
        c = pltpu.make_async_copy(bs.at[m], us.at[m], sem.at[m])
        c.start()
        copies.append(c)
    for m in range(4):
        bn[m] = tn[m] * cscn[m:m + 1, :]
    c = pltpu.make_async_copy(bn, un, sem.at[4])
    c.start()
    copies.append(c)
    for c in copies:
        c.wait()


def per_device(
    square_grads, narrow_grads, square_rowstate, square_colstate, narrow_rowstate, narrow_colstate
):
    hbm = pl.BlockSpec(memory_space=pltpu.HBM)
    vmem = pl.BlockSpec(memory_space=pltpu.VMEM)
    V = pltpu.VMEM
    middle = pl.pallas_call(
        exchange_kernel,
        out_shape=[
            jax.ShapeDtypeStruct((4, 128, 1024), f32), jax.ShapeDtypeStruct((4, 128, 128), f32),
            jax.ShapeDtypeStruct((8, 128), f32),
            jax.ShapeDtypeStruct((4, 1024), f32), jax.ShapeDtypeStruct((4, 128), f32),
            jax.ShapeDtypeStruct((4, 1024), f32), jax.ShapeDtypeStruct((4, 128), f32),
        ],
        in_specs=[hbm] * 6,
        out_specs=[vmem] * 7,
        scratch_shapes=[
            V((4, 128, 1024), jnp.bfloat16), V((4, 128, 128), jnp.bfloat16),
            V((4, 128), f32), V((4, 128), f32), V((4, 1024), f32), V((4, 128), f32),
            V((8, 128, 128), f32), V((8, 128, 128), f32),
            V((8, 8, 128), f32),
            V((OWNERS, CR, 128), f32), V((OWNERS, WR, 128), f32),
            V((16, CR, 128), f32), V((8, CR2, 128), f32),
            V((16, WR, 128), f32), V((8, WR2, 128), f32),
            V((2, CR, 128), f32), V((OWNERS, CR, 128), f32),
            V((4 * OWNERS, 2, 128), f32),
            pltpu.SemaphoreType.DMA((9,)),
            pltpu.SemaphoreType.DMA((7,)),
            pltpu.SemaphoreType.DMA((7,)),
        ],
        compiler_params=pltpu.CompilerParams(
            collective_id=0, has_side_effects=True, vmem_limit_bytes=24 * 2**20),
        name="exchange",
    )(*(pltpu.with_memory_space_constraint(a, pltpu.HBM) for a in (
        square_grads, narrow_grads, square_rowstate, narrow_rowstate, square_colstate, narrow_colstate)))
    us, un, rfs, cfs, rfn, cfn = pl.pallas_call(
        output_kernel,
        out_shape=[
            jax.ShapeDtypeStruct((4, 128, 1024), f32), jax.ShapeDtypeStruct((4, 128, 128), f32),
            jax.ShapeDtypeStruct((4, 128), f32), jax.ShapeDtypeStruct((4, 1024), f32),
            jax.ShapeDtypeStruct((4, 128), f32), jax.ShapeDtypeStruct((4, 128), f32),
        ],
        in_specs=[vmem] * 7,
        out_specs=[hbm] * 6,
        scratch_shapes=[
            V((4, 128, 1024), f32), V((4, 128, 128), f32), V((4, 128), f32), V((4, 128), f32),
            pltpu.SemaphoreType.DMA((9,)),
        ],
        compiler_params=pltpu.CompilerParams(vmem_limit_bytes=24 * 2**20),
        name="output",
    )(*middle)
    return us, un, rfs, cfs, rfn, cfn


def solution(mesh):
    torus = Mesh(mesh.devices.reshape(8, 8, 4, 2), ("wide_0", "wide_1", "narrow_0", "narrow_1"))
    in_specs = (
        P(None, WIDE, NARROW),
        P(None, WIDE, NARROW),
        P(None, WIDE),
        P(None, NARROW),
        P(None, WIDE),
        P(None, NARROW),
    )
    out_specs = (
        P(None, WIDE, NARROW),
        P(None, WIDE, NARROW),
        P(None, WIDE),
        P(None, NARROW),
        P(None, WIDE),
        P(None, NARROW),
    )
    return jax.shard_map(
        per_device, mesh=torus, in_specs=in_specs, out_specs=out_specs, check_vma=False
    )
```

```python
import functools

import jax
import jax.numpy as jnp
from jax import lax
from jax.experimental import pallas as pl
from jax.experimental.pallas import tpu as pltpu
from jax.sharding import Mesh
from jax.sharding import PartitionSpec as P

WIDE = ("wide_0", "wide_1")
NARROW = ("narrow_0", "narrow_1")
MESH = pl.DeviceIdType.MESH

decay_rate = 0.9
epsilon_square = 1e-30
clip_limit = 1.0

f32 = jnp.float32

ROWS, CZ, CY, WZ, AG, TX, SX = range(7)
FAR_FIRST = (4, 3, 5, 2, 6, 1, 7)

OWNERS = 2
OFFSET = 0
BLOCKS = 8 // OWNERS
NARROWS = max(1, 4 // OWNERS)
SQ = 4 * BLOCKS
CR = SQ + NARROWS
WR = CR + 1
CR2 = 2 * CR
WR2 = CR2 + 1
ROOT_ZS = (0, 1)
ROOTS = [(t_z, t_y, t_x) for t_y in (0, 1, 2, 3, 7, 4, 6, 5) for t_z in ROOT_ZS for t_x in (0, 1, 3, 2)]
SERVED = range(4) if len(ROOT_ZS) == 2 else (0, 1, 7, 2, 6, 3, 5, 4)


def exchange_kernel(
    gs, gn, rs, rn, cs, cn,
    ts, tn, rowf, colfs, colfn, cscs, cscn,
    vs, vn, vrs, vrn, vcs, vcn, part, rb,
    rows_buf, c_out, w_out, cz, cy, wz, w_all, own, ag, tx, sx,
    load_sem, send_sem, recv_sem,
):
    z, y = lax.axis_index("wide_0"), lax.axis_index("wide_1")
    x, core = lax.axis_index("narrow_0"), lax.axis_index("narrow_1")
    me = lax.rem(z + OFFSET, 8)
    on_plane = me < OWNERS
    is_owner = jnp.logical_and(on_plane, core == 1)
    is_root = jnp.logical_and(z < len(ROOT_ZS), core == 1)

    def on_y(d):
        return {"wide_1": lax.rem(y + d, 8)}

    def on_narrow(d):
        return {"narrow_0": lax.rem(x + d // 2, 4), "narrow_1": lax.rem(core + d % 2, 2)}

    barrier = pltpu.get_barrier_semaphore()
    for d in FAR_FIRST:
        pl.semaphore_signal(barrier, inc=1, device_id=on_narrow(d), device_id_type=MESH)

    loads = [pltpu.make_async_copy(gs.at[m], vs.at[m], load_sem.at[m]) for m in range(4)]
    loads.append(pltpu.make_async_copy(gn, vn, load_sem.at[4]))
    for i, (a, b) in enumerate(((rs, vrs), (rn, vrn), (cs, vcs), (cn, vcn))):
        loads.append(pltpu.make_async_copy(a, b, load_sem.at[5 + i]))
    for c in loads:
        c.start()

    @pl.when(is_owner)
    def _():
        for d in FAR_FIRST:
            for c in range(2):
                peer = {"wide_0": lax.rem(z + d, 8), "narrow_1": c}
                pl.semaphore_signal(barrier, inc=1, device_id=peer, device_id_type=MESH)
        for d in FAR_FIRST:
            pl.semaphore_signal(barrier, inc=1, device_id=on_y(d), device_id_type=MESH)

    def send(kind, src, dst, peer):
        pltpu.make_async_remote_copy(
            src_ref=src, dst_ref=dst, send_sem=send_sem.at[kind], recv_sem=recv_sem.at[kind],
            device_id=peer, device_id_type=MESH).start()

    def drained(kind, ref):
        pltpu.make_async_remote_copy(
            src_ref=ref, dst_ref=ref, send_sem=send_sem.at[kind], recv_sem=recv_sem.at[kind],
            device_id=on_y(1), device_id_type=MESH).wait_send()

    def arrived(kind, ref):
        pltpu.make_async_remote_copy(
            src_ref=ref, dst_ref=ref, send_sem=send_sem.at[kind], recv_sem=recv_sem.at[kind],
            device_id=on_y(1), device_id_type=MESH).wait_recv()

    def if_owner(then, otherwise):
        pl.when(is_owner)(then)
        pl.when(jnp.logical_not(is_owner))(otherwise)

    def to_owners(kind, out, buf):
        for d in FAR_FIRST + (0,):
            at = lax.rem(z + d, 8)
            o = lax.rem(at + OFFSET, 8)
            there = o < OWNERS

            @pl.when(there if d else jnp.logical_and(there, core == 0))
            def _():
                send(kind, out.at[o], buf.at[z * 2 + core], {"wide_0": at, "narrow_1": 1})

    def column_sums(m, ref, width):
        blocks = width // 128

        def step(r, acc):
            rows = pl.ds(r * 16, 16)
            v = ref[rows, :].astype(f32)
            q = v * v
            p = q[:, 0:128]
            for b in range(1, blocks):
                p = p + q[:, b * 128:(b + 1) * 128]
            part[m, rows, :] = p
            return acc + (q[0:8] + q[8:16])

        acc = lax.fori_loop(0, 8, step, jnp.zeros((8, width), f32), unroll=True)
        return jnp.sum(acc, axis=0, keepdims=True)

    def place_square(out, m, k, row):
        r = (k % BLOCKS) * 4 + m
        out[k // BLOCKS, r:r + 1, :] = row

    def place_narrow(out, m, row):
        for o in range(OWNERS):
            for i in range(NARROWS):
                if (o * NARROWS + i) % 4 == m:
                    out[o, SQ + i:SQ + i + 1, :] = row

    old = decay_rate / (1.0 - decay_rate) * 8192 / 64
    for m in range(4):
        loads[m].wait()
        if m == 0:
            for c in loads[5:]:
                c.wait()
        total = column_sums(m, vs.at[m], 1024) + old * vcs[m:m + 1, :]
        for k in range(8):
            place_square(c_out, m, k, total[:, k * 128:(k + 1) * 128])
    loads[4].wait()
    for m in range(4):
        place_narrow(c_out, m, column_sums(4 + m, vn.at[m], 128) + old * vcn[m:m + 1, :])
    for m in range(8):
        rows_buf[0, m:m + 1, :] = jnp.sum(part[m].T, axis=0, keepdims=True)

    others = jnp.where(on_plane, OWNERS - 1, OWNERS)
    pl.semaphore_wait(barrier, 7 + others + jnp.where(is_owner, 7, 0))

    for d in FAR_FIRST:
        send(ROWS, rows_buf.at[0], rows_buf.at[d], on_narrow(d))
    to_owners(CZ, c_out, cz)

    arrived(ROWS, rows_buf.at[pl.ds(1, 7)])
    rowsum = None
    for s_x in range(4):
        for s_c in range(2):
            slot = lax.rem(x + 4 - s_x, 4) * 2 + lax.rem(core + s_c, 2)
            piece = rows_buf[slot]
            rowsum = piece if rowsum is None else rowsum + piece
    sub = lax.broadcasted_iota(jnp.int32, (8, 128), 0)
    lane = lax.broadcasted_iota(jnp.int32, (8, 128), 1)
    rowf[0:4, :] = decay_rate * vrs[...] + (1.0 - decay_rate) * (rowsum[0:4] / 8192 + epsilon_square)
    rowf[4:8, :] = decay_rate * vrn[...] + (1.0 - decay_rate) * (rowsum[4:8] / 1024 + epsilon_square)
    factor = rowf[...]
    inverse = lax.rsqrt(factor)
    for m in range(8):
        rb[m] = jnp.broadcast_to(inverse[m:m + 1, :], (128, 128)).T
    totals = jnp.sum(factor, axis=1, keepdims=True)
    totals = jnp.sum(jnp.where(lane == sub + 8, totals, 0.0), axis=0, keepdims=True)
    for o in range(OWNERS):
        w_out[o, CR:CR + 1, :] = totals

    def weighted_sums(m, ref, out, width):
        blocks = width // 128

        def step(r, acc):
            rows = pl.ds(r * 16, 16)
            scale = rb[m, rows, :]
            v = ref[rows, :].astype(f32)
            new = []
            for b in range(blocks):
                t = v[:, b * 128:(b + 1) * 128] * scale
                out[rows, b * 128:(b + 1) * 128] = t
                q = t * t
                new.append(acc[b] + (q[0:8] + q[8:16]))
            return tuple(new)

        acc = lax.fori_loop(0, 8, step, tuple(jnp.zeros((8, 128), f32) for _ in range(blocks)), unroll=True)
        return [jnp.sum(a, axis=0, keepdims=True) for a in acc]

    for m in range(4):
        total = weighted_sums(m, vs.at[m], ts.at[m], 1024)
        for k in range(8):
            place_square(w_out, m, k, total[k])
    for m in range(4):
        place_narrow(w_out, m, weighted_sums(4 + m, vn.at[m], tn.at[m], 128)[0])
    to_owners(WZ, w_out, wz)

    def over_z(kind, out, buf, into, slot):
        arrived(kind, buf.at[pl.ds(0, 15)])
        for c in range(2):
            total = None
            for s in range(8):
                piece = jnp.where(jnp.logical_and(z == s, c == 1), out[me], buf[2 * s + c])
                total = piece if total is None else total + piece
            into[slot, SQ * c:SQ * c + SQ, :] = total[0:SQ]
            into[slot, 2 * SQ + NARROWS * c:2 * SQ + NARROWS * (c + 1), :] = total[SQ:CR]
        if kind == WZ:
            into[slot, CR2:WR2, :] = total[CR:WR]

    @pl.when(is_owner)
    def _():
        over_z(CZ, c_out, cz, cy, y)
        for d in FAR_FIRST:
            send(CY, cy.at[y], cy.at[y], on_y(d))
        arrived(CY, cy.at[pl.ds(0, 7)])
        colsum = cy[0]
        for s in range(1, 8):
            colsum = colsum + cy[s]
        colfactor = (1.0 - decay_rate) * (colsum / 8192 + epsilon_square)
        for c in range(2):
            own[c, 0:SQ, :] = colfactor[SQ * c:SQ * c + SQ]
            own[c, SQ:CR, :] = colfactor[2 * SQ + NARROWS * c:2 * SQ + NARROWS * (c + 1)]
        for d in FAR_FIRST + (0,):
            for c in range(2):
                if (d, c) != (0, 1):
                    send(AG, own.at[c], ag.at[me], {"wide_0": lax.rem(z + d, 8), "narrow_1": c})
        ag[me] = own[1]
        inverse = 1.0 / colfactor

        over_z(WZ, w_out, wz, w_all, 0)
        weighted = w_all[0]
        share = jnp.sum(weighted[0:CR2] * inverse, axis=1, keepdims=True)
        subc = lax.broadcasted_iota(jnp.int32, (CR2, 128), 0)
        lanec = lax.broadcasted_iota(jnp.int32, (CR2, 128), 1)
        narrow = 4 + me * NARROWS + lax.rem(subc - 2 * SQ, NARROWS)
        target = jnp.where(subc >= 2 * SQ, narrow, lax.rem(subc, 4))
        slot = (me * 8 + y) * 4 + x
        share = jnp.sum(jnp.where(lanec == target, share, 0.0), axis=0, keepdims=True)
        tx[slot] = share + weighted[CR2:WR2]
        mine = tx.at[slot]
        for t_z, t_y, t_x in ROOTS:
            @pl.when(jnp.logical_or(jnp.logical_or(z != t_z, y != t_y), x != t_x))
            def _():
                send(TX, mine, mine, {"wide_0": t_z, "wide_1": t_y, "narrow_0": t_x})

    def owner_arrived():
        if OWNERS > 1:
            arrived(AG, ag.at[pl.ds(0, OWNERS - 1)])

    if_owner(owner_arrived, lambda: arrived(AG, ag))
    for o in range(OWNERS):
        piece = ag[o]
        for b in range(BLOCKS):
            k = o * BLOCKS + b
            colfs[:, k * 128:(k + 1) * 128] = piece[4 * b:4 * b + 4]
        for i in range(NARROWS):
            if o * NARROWS + i < 4:
                colfn[o * NARROWS + i:o * NARROWS + i + 1, :] = piece[SQ + i:SQ + i + 1]
    inv_s, inv_n = lax.rsqrt(colfs[...]), lax.rsqrt(colfn[...])

    @pl.when(is_root)
    def _():
        arrived(TX, tx.at[pl.ds(0, 32 * OWNERS - 1)])
        sums = [tx[i] for i in range(4)]
        for i in range(4, 32 * OWNERS):
            sums[i % 4] = sums[i % 4] + tx[i]
        pair = (sums[0] + sums[1]) + (sums[2] + sums[3])
        entries = jnp.where(lane[0:1] < 4, 8192.0 * 8192.0, 8192.0 * 1024.0)
        row_mean = pltpu.roll(pair, 128 - 8, 1) / (4 * OWNERS * 8192)
        spread = jnp.sqrt(row_mean * pair / entries)
        sx[...] = jnp.sqrt(row_mean) / jnp.maximum(1.0, spread / clip_limit)
        for i in SERVED:
            for c in (1, 0):
                if (i, c) != (0, 1):
                    at = z + i if len(ROOT_ZS) == 1 else z + 8 + i * (2 * z - 1)
                    send(SX, sx, sx, {"wide_0": lax.rem(at, 8), "narrow_1": c})

    @pl.when(jnp.logical_not(is_root))
    def _():
        arrived(SX, sx)

    scale = jnp.sum(jnp.where(lane == sub, jnp.broadcast_to(sx[...], (8, 128)), 0.0), axis=1, keepdims=True)
    cscs[...] = inv_s * scale[0:4]
    cscn[...] = inv_n * scale[4:8]

    drained(ROWS, rows_buf.at[pl.ds(1, 7)])

    def drain_owner():
        if OWNERS > 1:
            drained(CZ, c_out.at[pl.ds(0, OWNERS - 1)])
            drained(WZ, w_out.at[pl.ds(0, OWNERS - 1)])
        drained(CY, cy.at[pl.ds(0, 7)])
        drained(AG, cz.at[pl.ds(0, 15)])

        @pl.when(is_root)
        def _():
            drained(TX, tx.at[pl.ds(0, len(ROOTS) - 1)])
            drained(SX, part.at[0, pl.ds(0, 2 * len(SERVED) - 1)])

        @pl.when(jnp.logical_not(is_root))
        def _():
            drained(TX, tx.at[pl.ds(0, len(ROOTS))])

    def drain_other():
        drained(CZ, c_out)
        drained(WZ, w_out)

    if_owner(drain_owner, drain_other)


def output_kernel(
    ts, tn, rowf, colfs, colfn, cscs, cscn,
    us, un, rfs, cfs, rfn, cfn,
    bs, bn, brs, brn, sem,
):
    brs[...] = rowf[0:4, :]
    brn[...] = rowf[4:8, :]
    copies = [
        pltpu.make_async_copy(brs, rfs, sem.at[5]),
        pltpu.make_async_copy(brn, rfn, sem.at[6]),
        pltpu.make_async_copy(colfs, cfs, sem.at[7]),
        pltpu.make_async_copy(colfn, cfn, sem.at[8]),
    ]
    for c in copies:
        c.start()
    for m in range(4):
        bs[m] = ts[m] * cscs[m:m + 1, :]
        c = pltpu.make_async_copy(bs.at[m], us.at[m], sem.at[m])
        c.start()
        copies.append(c)
    for m in range(4):
        bn[m] = tn[m] * cscn[m:m + 1, :]
    c = pltpu.make_async_copy(bn, un, sem.at[4])
    c.start()
    copies.append(c)
    for c in copies:
        c.wait()


def per_device(
    square_grads, narrow_grads, square_rowstate, square_colstate, narrow_rowstate, narrow_colstate
):
    hbm = pl.BlockSpec(memory_space=pltpu.HBM)
    vmem = pl.BlockSpec(memory_space=pltpu.VMEM)
    V = pltpu.VMEM
    middle = pl.pallas_call(
        exchange_kernel,
        out_shape=[
            jax.ShapeDtypeStruct((4, 128, 1024), f32), jax.ShapeDtypeStruct((4, 128, 128), f32),
            jax.ShapeDtypeStruct((8, 128), f32),
            jax.ShapeDtypeStruct((4, 1024), f32), jax.ShapeDtypeStruct((4, 128), f32),
            jax.ShapeDtypeStruct((4, 1024), f32), jax.ShapeDtypeStruct((4, 128), f32),
        ],
        in_specs=[hbm] * 6,
        out_specs=[vmem] * 7,
        scratch_shapes=[
            V((4, 128, 1024), jnp.bfloat16), V((4, 128, 128), jnp.bfloat16),
            V((4, 128), f32), V((4, 128), f32), V((4, 1024), f32), V((4, 128), f32),
            V((8, 128, 128), f32), V((8, 128, 128), f32),
            V((8, 8, 128), f32),
            V((OWNERS, CR, 128), f32), V((OWNERS, WR, 128), f32),
            V((16, CR, 128), f32), V((8, CR2, 128), f32),
            V((16, WR, 128), f32), V((1, WR2, 128), f32),
            V((2, CR, 128), f32), V((OWNERS, CR, 128), f32),
            V((32 * OWNERS, 1, 128), f32), V((1, 128), f32),
            pltpu.SemaphoreType.DMA((9,)),
            pltpu.SemaphoreType.DMA((7,)),
            pltpu.SemaphoreType.DMA((7,)),
        ],
        compiler_params=pltpu.CompilerParams(
            collective_id=0, has_side_effects=True, vmem_limit_bytes=24 * 2**20),
        name="exchange",
    )(*(pltpu.with_memory_space_constraint(a, pltpu.HBM) for a in (
        square_grads, narrow_grads, square_rowstate, narrow_rowstate, square_colstate, narrow_colstate)))
    us, un, rfs, cfs, rfn, cfn = pl.pallas_call(
        output_kernel,
        out_shape=[
            jax.ShapeDtypeStruct((4, 128, 1024), f32), jax.ShapeDtypeStruct((4, 128, 128), f32),
            jax.ShapeDtypeStruct((4, 128), f32), jax.ShapeDtypeStruct((4, 1024), f32),
            jax.ShapeDtypeStruct((4, 128), f32), jax.ShapeDtypeStruct((4, 128), f32),
        ],
        in_specs=[vmem] * 7,
        out_specs=[hbm] * 6,
        scratch_shapes=[
            V((4, 128, 1024), f32), V((4, 128, 128), f32), V((4, 128), f32), V((4, 128), f32),
            pltpu.SemaphoreType.DMA((9,)),
        ],
        compiler_params=pltpu.CompilerParams(vmem_limit_bytes=24 * 2**20),
        name="output",
    )(*middle)
    return us, un, rfs, cfs, rfn, cfn


def solution(mesh):
    torus = Mesh(mesh.devices.reshape(8, 8, 4, 2), ("wide_0", "wide_1", "narrow_0", "narrow_1"))
    in_specs = (
        P(None, WIDE, NARROW),
        P(None, WIDE, NARROW),
        P(None, WIDE),
        P(None, NARROW),
        P(None, WIDE),
        P(None, NARROW),
    )
    out_specs = (
        P(None, WIDE, NARROW),
        P(None, WIDE, NARROW),
        P(None, WIDE),
        P(None, NARROW),
        P(None, WIDE),
        P(None, NARROW),
    )
    return jax.shard_map(
        per_device, mesh=torus, in_specs=in_specs, out_specs=out_specs, check_vma=False
    )
```

```python
import functools

import jax
import jax.numpy as jnp
from jax import lax
from jax.experimental import pallas as pl
from jax.experimental.pallas import tpu as pltpu
from jax.sharding import Mesh
from jax.sharding import PartitionSpec as P

WIDE = ("wide_0", "wide_1")
NARROW = ("narrow_0", "narrow_1")
MESH = pl.DeviceIdType.MESH

decay_rate = 0.9
epsilon_square = 1e-30
clip_limit = 1.0

f32 = jnp.float32

ROWS, CZ, CY, WZ, AG, TX, SX = range(7)
FAR_FIRST = (4, 3, 5, 2, 6, 1, 7)
NARROW_FAR_FIRST = (5, 4, 3, 7, 2, 6, 1)

OWNERS = 2
OFFSET = 0
BLOCKS = 8 // OWNERS
NARROWS = max(1, 4 // OWNERS)
SQ = 4 * BLOCKS
CR = SQ + NARROWS
WR = CR + 1
CR2 = 2 * CR
WR2 = CR2 + 1
ROOTS = [root for t_y in (0, 1, 2, 3, 7, 4, 6, 5) for root in
         [(0, t_y, t_x, 1) for t_x in (0, 1, 3, 2)]
         + [(0, t_y, t_x, 0) for t_x in (0, 1, 3, 2)]
         + [(1, t_y, t_x, 1) for t_x in (0, 1, 3, 2)]]
SERVED = [(1, 0)] + [(t_z, t_c) for t_z in (2, 7, 3, 6, 4, 5) for t_c in (1, 0)]


def exchange_kernel(
    gs, gn, rs, rn, cs, cn,
    ts, tn, rowf, colfs, colfn, cscs, cscn,
    vs, vn, vrs, vrn, vcs, vcn, qs, qn, part, rb,
    rows_buf, c_out, w_out, cz, cy, wz, w_all, own, ag, tx, sx,
    load_sem, send_sem, recv_sem,
):
    z, y = lax.axis_index("wide_0"), lax.axis_index("wide_1")
    x, core = lax.axis_index("narrow_0"), lax.axis_index("narrow_1")
    me = lax.rem(z + OFFSET, 8)
    on_plane = me < OWNERS
    is_owner = jnp.logical_and(on_plane, core == 1)
    is_server = jnp.logical_and(z == 1, core == 1)
    is_root = jnp.logical_or(z == 0, is_server)

    def on_y(d):
        return {"wide_1": lax.rem(y + d, 8)}

    def on_narrow(d):
        return {"narrow_0": lax.rem(x + d // 2, 4), "narrow_1": lax.rem(core + d % 2, 2)}

    barrier = pltpu.get_barrier_semaphore()
    for d in NARROW_FAR_FIRST:
        pl.semaphore_signal(barrier, inc=1, device_id=on_narrow(d), device_id_type=MESH)

    loads = [pltpu.make_async_copy(gs.at[m], vs.at[m], load_sem.at[m]) for m in range(4)]
    loads.append(pltpu.make_async_copy(gn, vn, load_sem.at[4]))
    for i, (a, b) in enumerate(((rs, vrs), (rn, vrn), (cs, vcs), (cn, vcn))):
        loads.append(pltpu.make_async_copy(a, b, load_sem.at[5 + i]))
    for c in loads:
        c.start()

    @pl.when(is_owner)
    def _():
        for d in FAR_FIRST:
            for c in range(2):
                peer = {"wide_0": lax.rem(z + d, 8), "narrow_1": c}
                pl.semaphore_signal(barrier, inc=1, device_id=peer, device_id_type=MESH)
        for d in FAR_FIRST:
            pl.semaphore_signal(barrier, inc=1, device_id=on_y(d), device_id_type=MESH)

    def send(kind, src, dst, peer):
        pltpu.make_async_remote_copy(
            src_ref=src, dst_ref=dst, send_sem=send_sem.at[kind], recv_sem=recv_sem.at[kind],
            device_id=peer, device_id_type=MESH).start()

    def drained(kind, ref):
        pltpu.make_async_remote_copy(
            src_ref=ref, dst_ref=ref, send_sem=send_sem.at[kind], recv_sem=recv_sem.at[kind],
            device_id=on_y(1), device_id_type=MESH).wait_send()

    def arrived(kind, ref):
        pltpu.make_async_remote_copy(
            src_ref=ref, dst_ref=ref, send_sem=send_sem.at[kind], recv_sem=recv_sem.at[kind],
            device_id=on_y(1), device_id_type=MESH).wait_recv()

    def if_owner(then, otherwise):
        pl.when(is_owner)(then)
        pl.when(jnp.logical_not(is_owner))(otherwise)

    def to_owners(kind, out, buf):
        for d in FAR_FIRST + (0,):
            at = lax.rem(z + d, 8)
            o = lax.rem(at + OFFSET, 8)
            there = o < OWNERS

            @pl.when(there if d else jnp.logical_and(there, core == 0))
            def _():
                send(kind, out.at[o], buf.at[z * 2 + core], {"wide_0": at, "narrow_1": 1})

    def row_sums(m, ref, out, width):
        blocks = width // 128
        for r in range(8):
            rows = pl.ds(r * 16, 16)
            p = None
            for b in range(blocks):
                v = ref[rows, b * 128:(b + 1) * 128].astype(f32)
                q = v * v
                out[rows, b * 128:(b + 1) * 128] = q
                p = q if p is None else p + q
            part[m, rows, :] = p
        rows_buf[0, m:m + 1, :] = jnp.sum(part[m].T, axis=0, keepdims=True)

    def place_square(out, m, k, row):
        r = (k % BLOCKS) * 4 + m
        out[k // BLOCKS, r:r + 1, :] = row

    def place_narrow(out, m, row):
        for o in range(OWNERS):
            for i in range(NARROWS):
                if (o * NARROWS + i) % 4 == m:
                    out[o, SQ + i:SQ + i + 1, :] = row

    for m in range(4):
        loads[m].wait()
        row_sums(m, vs.at[m], qs.at[m], 1024)
    loads[4].wait()
    for m in range(4):
        row_sums(4 + m, vn.at[m], qn.at[m], 128)

    others = jnp.where(on_plane, OWNERS - 1, OWNERS)
    pl.semaphore_wait(barrier, 7 + others + jnp.where(is_owner, 7, 0))

    for d in NARROW_FAR_FIRST:
        send(ROWS, rows_buf.at[0], rows_buf.at[d], on_narrow(d))

    def column_sums(ref, width, weight=None):
        acc = [None] * (width // 128)
        for r in range(16):
            rows = pl.ds(r * 8, 8)
            w = None if weight is None else weight[rows, :] * weight[rows, :]
            for b in range(width // 128):
                q = ref[rows, b * 128:(b + 1) * 128]
                q = q if w is None else q * w
                acc[b] = q if acc[b] is None else acc[b] + q
        return [jnp.sum(a, axis=0, keepdims=True) for a in acc]

    for c in loads[5:]:
        c.wait()
    old = decay_rate / (1.0 - decay_rate) * 8192 / 64
    for m in range(4):
        total = column_sums(qs.at[m], 1024)
        for k in range(8):
            place_square(c_out, m, k, total[k] + old * vcs[m:m + 1, k * 128:(k + 1) * 128])
    for m in range(4):
        place_narrow(c_out, m, column_sums(qn.at[m], 128)[0] + old * vcn[m:m + 1, :])
    to_owners(CZ, c_out, cz)

    arrived(ROWS, rows_buf.at[pl.ds(1, 7)])
    rowsum = None
    for s_x in range(4):
        for s_c in range(2):
            slot = lax.rem(x + 4 - s_x, 4) * 2 + lax.rem(core + s_c, 2)
            piece = rows_buf[slot]
            rowsum = piece if rowsum is None else rowsum + piece
    sub = lax.broadcasted_iota(jnp.int32, (8, 128), 0)
    lane = lax.broadcasted_iota(jnp.int32, (8, 128), 1)
    rowf[0:4, :] = decay_rate * vrs[...] + (1.0 - decay_rate) * (rowsum[0:4] / 8192 + epsilon_square)
    rowf[4:8, :] = decay_rate * vrn[...] + (1.0 - decay_rate) * (rowsum[4:8] / 1024 + epsilon_square)
    factor = rowf[...]
    inverse = lax.rsqrt(factor)
    for m in range(8):
        rb[m] = jnp.broadcast_to(inverse[m:m + 1, :], (128, 128)).T
    totals = jnp.sum(factor, axis=1, keepdims=True)
    totals = jnp.sum(jnp.where(lane == sub + 8, totals, 0.0), axis=0, keepdims=True)
    for o in range(OWNERS):
        w_out[o, CR:CR + 1, :] = totals

    for m in range(4):
        total = column_sums(qs.at[m], 1024, rb.at[m])
        for k in range(8):
            place_square(w_out, m, k, total[k])
    for m in range(4):
        place_narrow(w_out, m, column_sums(qn.at[m], 128, rb.at[4 + m])[0])
    to_owners(WZ, w_out, wz)
    for m in range(8):
        for r in range(8):
            rows = pl.ds(r * 16, 16)
            scale = rb[m, rows, :]
            if m < 4:
                for b in range(8):
                    columns = slice(b * 128, (b + 1) * 128)
                    ts[m, rows, columns] = vs[m, rows, columns].astype(f32) * scale
            else:
                tn[m - 4, rows, :] = vn[m - 4, rows, :].astype(f32) * scale

    def over_z(kind, out, buf, into, slot):
        arrived(kind, buf.at[pl.ds(0, 15)])
        for c in range(2):
            total = None
            for s in range(8):
                piece = jnp.where(jnp.logical_and(z == s, c == 1), out[me], buf[2 * s + c])
                total = piece if total is None else total + piece
            into[slot, SQ * c:SQ * c + SQ, :] = total[0:SQ]
            into[slot, 2 * SQ + NARROWS * c:2 * SQ + NARROWS * (c + 1), :] = total[SQ:CR]
        if kind == WZ:
            into[slot, CR2:WR2, :] = total[CR:WR]

    @pl.when(is_owner)
    def _():
        over_z(CZ, c_out, cz, cy, y)
        for d in FAR_FIRST:
            send(CY, cy.at[y], cy.at[y], on_y(d))
        arrived(CY, cy.at[pl.ds(0, 7)])
        colsum = cy[0]
        for s in range(1, 8):
            colsum = colsum + cy[s]
        colfactor = (1.0 - decay_rate) * (colsum / 8192 + epsilon_square)
        for c in range(2):
            own[c, 0:SQ, :] = colfactor[SQ * c:SQ * c + SQ]
            own[c, SQ:CR, :] = colfactor[2 * SQ + NARROWS * c:2 * SQ + NARROWS * (c + 1)]
        for d in FAR_FIRST + (0,):
            for c in range(2):
                if (d, c) != (0, 1):
                    send(AG, own.at[c], ag.at[me], {"wide_0": lax.rem(z + d, 8), "narrow_1": c})
        ag[me] = own[1]
        inverse = 1.0 / colfactor

        over_z(WZ, w_out, wz, w_all, 0)
        weighted = w_all[0]
        share = jnp.sum(weighted[0:CR2] * inverse, axis=1, keepdims=True)
        subc = lax.broadcasted_iota(jnp.int32, (CR2, 128), 0)
        lanec = lax.broadcasted_iota(jnp.int32, (CR2, 128), 1)
        narrow = 4 + me * NARROWS + lax.rem(subc - 2 * SQ, NARROWS)
        target = jnp.where(subc >= 2 * SQ, narrow, lax.rem(subc, 4))
        slot = (me * 8 + y) * 4 + x
        share = jnp.sum(jnp.where(lanec == target, share, 0.0), axis=0, keepdims=True)
        tx[slot] = share + weighted[CR2:WR2]
        mine = tx.at[slot]
        for t_z, t_y, t_x, t_c in ROOTS:
            peer = {"wide_0": t_z, "wide_1": t_y, "narrow_0": t_x, "narrow_1": t_c}
            if t_c == 0:
                send(TX, mine, mine, peer)
            else:
                @pl.when(jnp.logical_or(jnp.logical_or(z != t_z, y != t_y), x != t_x))
                def _():
                    send(TX, mine, mine, peer)

    def owner_arrived():
        if OWNERS > 1:
            arrived(AG, ag.at[pl.ds(0, OWNERS - 1)])

    if_owner(owner_arrived, lambda: arrived(AG, ag))
    for o in range(OWNERS):
        piece = ag[o]
        for b in range(BLOCKS):
            k = o * BLOCKS + b
            colfs[:, k * 128:(k + 1) * 128] = piece[4 * b:4 * b + 4]
        for i in range(NARROWS):
            if o * NARROWS + i < 4:
                colfn[o * NARROWS + i:o * NARROWS + i + 1, :] = piece[SQ + i:SQ + i + 1]
    inv_s, inv_n = lax.rsqrt(colfs[...]), lax.rsqrt(colfn[...])

    @pl.when(is_root)
    def _():
        if_owner(lambda: arrived(TX, tx.at[pl.ds(0, 32 * OWNERS - 1)]), lambda: arrived(TX, tx))
        sums = [tx[i] for i in range(4)]
        for i in range(4, 32 * OWNERS):
            sums[i % 4] = sums[i % 4] + tx[i]
        pair = (sums[0] + sums[1]) + (sums[2] + sums[3])
        entries = jnp.where(lane[0:1] < 4, 8192.0 * 8192.0, 8192.0 * 1024.0)
        row_mean = pltpu.roll(pair, 128 - 8, 1) / (4 * OWNERS * 8192)
        spread = jnp.sqrt(row_mean * pair / entries)
        sx[...] = jnp.sqrt(row_mean) / jnp.maximum(1.0, spread / clip_limit)

        @pl.when(is_server)
        def _():
            for t_z, t_c in SERVED:
                send(SX, sx, sx, {"wide_0": t_z, "narrow_1": t_c})

    @pl.when(jnp.logical_not(is_root))
    def _():
        arrived(SX, sx)

    scale = jnp.sum(jnp.where(lane == sub, jnp.broadcast_to(sx[...], (8, 128)), 0.0), axis=1, keepdims=True)
    cscs[...] = inv_s * scale[0:4]
    cscn[...] = inv_n * scale[4:8]

    drained(ROWS, rows_buf.at[pl.ds(1, 7)])

    def drain_owner():
        if OWNERS > 1:
            drained(CZ, c_out.at[pl.ds(0, OWNERS - 1)])
            drained(WZ, w_out.at[pl.ds(0, OWNERS - 1)])
        drained(CY, cy.at[pl.ds(0, 7)])
        drained(AG, cz.at[pl.ds(0, 15)])

        drained(TX, part.at[0, pl.ds(0, len(ROOTS) - 1)])

        @pl.when(is_server)
        def _():
            drained(SX, part.at[0, pl.ds(0, len(SERVED))])

    def drain_other():
        drained(CZ, c_out)
        drained(WZ, w_out)

    if_owner(drain_owner, drain_other)


def output_kernel(
    ts, tn, rowf, colfs, colfn, cscs, cscn,
    us, un, rfs, cfs, rfn, cfn,
    bs, bn, brs, brn, sem,
):
    brs[...] = rowf[0:4, :]
    brn[...] = rowf[4:8, :]
    copies = [
        pltpu.make_async_copy(brs, rfs, sem.at[5]),
        pltpu.make_async_copy(brn, rfn, sem.at[6]),
        pltpu.make_async_copy(colfs, cfs, sem.at[7]),
        pltpu.make_async_copy(colfn, cfn, sem.at[8]),
    ]
    for c in copies:
        c.start()
    for m in range(4):
        bs[m] = ts[m] * cscs[m:m + 1, :]
        c = pltpu.make_async_copy(bs.at[m], us.at[m], sem.at[m])
        c.start()
        copies.append(c)
    for m in range(4):
        bn[m] = tn[m] * cscn[m:m + 1, :]
    c = pltpu.make_async_copy(bn, un, sem.at[4])
    c.start()
    copies.append(c)
    for c in copies:
        c.wait()


def per_device(
    square_grads, narrow_grads, square_rowstate, square_colstate, narrow_rowstate, narrow_colstate
):
    hbm = pl.BlockSpec(memory_space=pltpu.HBM)
    vmem = pl.BlockSpec(memory_space=pltpu.VMEM)
    V = pltpu.VMEM
    middle = pl.pallas_call(
        exchange_kernel,
        out_shape=[
            jax.ShapeDtypeStruct((4, 128, 1024), f32), jax.ShapeDtypeStruct((4, 128, 128), f32),
            jax.ShapeDtypeStruct((8, 128), f32),
            jax.ShapeDtypeStruct((4, 1024), f32), jax.ShapeDtypeStruct((4, 128), f32),
            jax.ShapeDtypeStruct((4, 1024), f32), jax.ShapeDtypeStruct((4, 128), f32),
        ],
        in_specs=[hbm] * 6,
        out_specs=[vmem] * 7,
        scratch_shapes=[
            V((4, 128, 1024), jnp.bfloat16), V((4, 128, 128), jnp.bfloat16),
            V((4, 128), f32), V((4, 128), f32), V((4, 1024), f32), V((4, 128), f32),
            V((4, 128, 1024), f32), V((4, 128, 128), f32),
            V((8, 128, 128), f32), V((8, 128, 128), f32),
            V((8, 8, 128), f32),
            V((OWNERS, CR, 128), f32), V((OWNERS, WR, 128), f32),
            V((16, CR, 128), f32), V((8, CR2, 128), f32),
            V((16, WR, 128), f32), V((1, WR2, 128), f32),
            V((2, CR, 128), f32), V((OWNERS, CR, 128), f32),
            V((32 * OWNERS, 1, 128), f32), V((1, 128), f32),
            pltpu.SemaphoreType.DMA((9,)),
            pltpu.SemaphoreType.DMA((7,)),
            pltpu.SemaphoreType.DMA((7,)),
        ],
        compiler_params=pltpu.CompilerParams(
            collective_id=0, has_side_effects=True, vmem_limit_bytes=24 * 2**20),
        name="exchange",
    )(*(pltpu.with_memory_space_constraint(a, pltpu.HBM) for a in (
        square_grads, narrow_grads, square_rowstate, narrow_rowstate, square_colstate, narrow_colstate)))
    us, un, rfs, cfs, rfn, cfn = pl.pallas_call(
        output_kernel,
        out_shape=[
            jax.ShapeDtypeStruct((4, 128, 1024), f32), jax.ShapeDtypeStruct((4, 128, 128), f32),
            jax.ShapeDtypeStruct((4, 128), f32), jax.ShapeDtypeStruct((4, 1024), f32),
            jax.ShapeDtypeStruct((4, 128), f32), jax.ShapeDtypeStruct((4, 128), f32),
        ],
        in_specs=[vmem] * 7,
        out_specs=[hbm] * 6,
        scratch_shapes=[
            V((4, 128, 1024), f32), V((4, 128, 128), f32), V((4, 128), f32), V((4, 128), f32),
            pltpu.SemaphoreType.DMA((9,)),
        ],
        compiler_params=pltpu.CompilerParams(vmem_limit_bytes=24 * 2**20),
        name="output",
    )(*middle)
    return us, un, rfs, cfs, rfn, cfn


def solution(mesh):
    torus = Mesh(mesh.devices.reshape(8, 8, 4, 2), ("wide_0", "wide_1", "narrow_0", "narrow_1"))
    in_specs = (
        P(None, WIDE, NARROW),
        P(None, WIDE, NARROW),
        P(None, WIDE),
        P(None, NARROW),
        P(None, WIDE),
        P(None, NARROW),
    )
    out_specs = (
        P(None, WIDE, NARROW),
        P(None, WIDE, NARROW),
        P(None, WIDE),
        P(None, NARROW),
        P(None, WIDE),
        P(None, NARROW),
    )
    return jax.shard_map(
        per_device, mesh=torus, in_specs=in_specs, out_specs=out_specs, check_vma=False
    )
```
